8 devices in a mesh: dz: 2 (over z, y), dy: 2 (over x), dx: 2 (over core).
Axes of the slice: x: 2, y: 2, z: 1, core: 2. Of those that a mesh axis runs over, the one named last changes fastest.
Arguments:
- x: bfloat16 [16384, 2048], P(('dx', 'dy', 'dz'))
- g: bfloat16 [16384, 2048], P(('dx', 'dy', 'dz'))
- w1: bfloat16 [2048, 8192], replicated
- w2: bfloat16 [8192, 2048], replicated
- w3: bfloat16 [2048, 8192], replicated
- w4: bfloat16 [8192, 2048], replicated
- m1: float32 [2048, 8192], P(('dx', 'dy', 'dz'))
- m2: float32 [8192, 2048], P(('dx', 'dy', 'dz'))
- m3: float32 [2048, 8192], P(('dx', 'dy', 'dz'))
- m4: float32 [8192, 2048], P(('dx', 'dy', 'dz'))
Outputs:
- output 1: bfloat16 [16384, 2048], P(('dx', 'dy', 'dz'))
- output 2: bfloat16 [2048, 8192], replicated
- output 3: bfloat16 [8192, 2048], replicated
- output 4: bfloat16 [2048, 8192], replicated
- output 5: bfloat16 [8192, 2048], replicated
- output 6: float32 [2048, 8192], P(('dx', 'dy', 'dz'))
- output 7: float32 [8192, 2048], P(('dx', 'dy', 'dz'))
- output 8: float32 [2048, 8192], P(('dx', 'dy', 'dz'))
- output 9: float32 [8192, 2048], P(('dx', 'dy', 'dz'))
All inputs are finite; a program needn't handle non-finite values.
Results may differ from the reference program's by a relative error of at most 0.010999.
Values are sent between devices in bfloat16 or wider.
A program may use at most 1.5 GiB of HBM per device.

```python
import jax
import jax.numpy as jnp
from jax import lax

D = 2048
F = 8192
TOKENS_DEV = 2048
DEVICES = 8
TOKENS = TOKENS_DEV * DEVICES
LR = 0.0005
MU = 0.9


def setup_inputs(seed: int = 0) -> dict:
    ks = jax.random.split(jax.random.key(seed), 10)
    f32 = jnp.float32
    ms = 0.3 * (TOKENS_DEV / DEVICES) ** 0.5
    x = jax.random.normal(ks[0], (TOKENS, D), f32)
    g = jax.random.normal(ks[1], (TOKENS, D), f32)
    w1 = jax.random.normal(ks[2], (D, F), f32) * D ** -0.5
    w2 = jax.random.normal(ks[3], (F, D), f32) * F ** -0.5
    w3 = jax.random.normal(ks[4], (D, F), f32) * D ** -0.5
    w4 = jax.random.normal(ks[5], (F, D), f32) * F ** -0.5
    m1 = jax.random.normal(ks[6], (D, F), f32) * ms
    m2 = jax.random.normal(ks[7], (F, D), f32) * ms
    m3 = jax.random.normal(ks[8], (D, F), f32) * ms
    m4 = jax.random.normal(ks[9], (F, D), f32) * ms
    bf = jnp.bfloat16
    return {"x": x.astype(bf), "g": g.astype(bf), "w1": w1.astype(bf), "w2": w2.astype(bf),
            "w3": w3.astype(bf), "w4": w4.astype(bf), "m1": m1, "m2": m2, "m3": m3, "m4": m4}


def _gelu(z):
    return jax.nn.gelu(z, approximate=True)


def _gelu_grad(z, dh):
    return jax.vjp(_gelu, z.astype(jnp.float32))[1](dh.astype(jnp.float32))[0]


def _device_pass(x, g, w1, w2, w3, w4):
    f32, bf = jnp.float32, jnp.bfloat16
    z1 = jnp.dot(x, w1, preferred_element_type=f32).astype(bf)
    h1 = _gelu(z1.astype(f32)).astype(bf)
    h2 = (jnp.dot(h1, w2, preferred_element_type=f32) + x.astype(f32)).astype(bf)
    z3 = jnp.dot(h2, w3, preferred_element_type=f32).astype(bf)
    h3 = _gelu(z3.astype(f32)).astype(bf)
    s4 = jnp.dot(h3.T, g, preferred_element_type=f32)
    dh3 = jnp.dot(g, w4.T, preferred_element_type=f32).astype(bf)
    dz3 = _gelu_grad(z3, dh3).astype(bf)
    s3 = jnp.dot(h2.T, dz3, preferred_element_type=f32)
    dh2 = (jnp.dot(dz3, w3.T, preferred_element_type=f32) + g.astype(f32)).astype(bf)
    s2 = jnp.dot(h1.T, dh2, preferred_element_type=f32)
    dh1 = jnp.dot(dh2, w2.T, preferred_element_type=f32).astype(bf)
    dz1 = _gelu_grad(z1, dh1).astype(bf)
    s1 = jnp.dot(x.T, dz1, preferred_element_type=f32)
    dx = (jnp.dot(dz1, w1.T, preferred_element_type=f32) + dh2.astype(f32)).astype(bf)
    return dx, (s1, s2, s3, s4)


def reference(x, g, w1, w2, w3, w4, m1, m2, m3, m4):
    f32, bf = jnp.float32, jnp.bfloat16
    xs = x.reshape(DEVICES, TOKENS_DEV, D)
    gs = g.reshape(DEVICES, TOKENS_DEV, D)

    def step(acc, xg):
        dxd, ss = _device_pass(xg[0], xg[1], w1, w2, w3, w4)
        return tuple(a + s for a, s in zip(acc, ss)), dxd

    zeros = (jnp.zeros((D, F), f32), jnp.zeros((F, D), f32), jnp.zeros((D, F), f32), jnp.zeros((F, D), f32))
    acc, dxs = lax.scan(step, zeros, (xs, gs))
    m1n = MU * m1 + acc[0] / DEVICES
    m2n = MU * m2 + acc[1] / DEVICES
    m3n = MU * m3 + acc[2] / DEVICES
    m4n = MU * m4 + acc[3] / DEVICES
    w1n = (w1.astype(f32) - LR * m1n).astype(bf)
    w2n = (w2.astype(f32) - LR * m2n).astype(bf)
    w3n = (w3.astype(f32) - LR * m3n).astype(bf)
    w4n = (w4.astype(f32) - LR * m4n).astype(bf)
    dx = dxs.reshape(TOKENS, D)
    return (dx, w1n, w2n, w3n, w4n, m1n, m2n, m3n, m4n)
```

```python
import jax
import jax.numpy as jnp
from jax import lax
from jax.experimental import pallas as pl
from jax.experimental.layout import Layout, with_layout_constraint
from jax.sharding import PartitionSpec as P


LR = 0.0005
MU = 0.9
DATA = ("dx", "dy", "dz")


def _gelu(z):
    return jax.nn.gelu(z, approximate=True)


def _gelu_grad(z, dh):
    return jax.vjp(_gelu, z.astype(jnp.float32))[1](dh.astype(jnp.float32))[0]


def _row_major(a):
    return with_layout_constraint(a, Layout(major_to_minor=(0, 1)))


def _copy_block(src, dst):
    dst[...] = src[...]


def _copy(a):
    r, c = a.shape
    spec = pl.BlockSpec(((1 << 20) // c, c), lambda b: (b, 0))
    return pl.pallas_call(_copy_block, grid=(r * c >> 20,), in_specs=[spec], out_specs=spec,
                          out_shape=jax.ShapeDtypeStruct(a.shape, a.dtype),
                          cost_estimate=pl.CostEstimate(flops=r * c, bytes_accessed=4 * r * c, transcendentals=0))(a)


def solution(mesh):
    ndx, ndy, ndz = mesh.shape["dx"], mesh.shape["dy"], mesh.shape["dz"]
    n = ndx * ndy * ndz
    f32, bf = jnp.float32, jnp.bfloat16
    swap = [(0, 1), (1, 0)]

    def nt(a, b):
        return lax.dot_general(a, b, (((1,), (1,)), ((), ())), preferred_element_type=f32)

    def tn(a, b):
        return lax.dot_general(a, b, (((0,), (0,)), ((), ())), preferred_element_type=f32)

    def nn(a, b):
        return jnp.dot(a, b, preferred_element_type=f32)

    def act(z):
        return _gelu(z.astype(f32)).astype(bf)

    def body(x, g, w1, w2, w3, w4, m1, m2, m3, m4):
        i, j, k = lax.axis_index("dx"), lax.axis_index("dy"), lax.axis_index("dz")
        q, qp = 2 * i + j, 2 * (1 - i) + j
        d, f = w1.shape
        fq = f // 4

        def cols(a, b):
            return lax.dynamic_slice_in_dim(a, b * fq, fq, 1)

        def rows(a, b):
            return lax.dynamic_slice_in_dim(a, b * fq, fq, 0)

        def send(a, ax):
            return lax.ppermute(a, ax, swap)

        def both(a):
            return lax.all_gather(a, "dx", axis=0, tiled=True)

        def sum_f(s):
            half = fq // 2
            r = send(lax.dynamic_slice_in_dim(s, (1 - k) * half, half, 0), "dz")
            return lax.dynamic_slice_in_dim(s, k * half, half, 0) + r

        def sum_d(s):
            s = s.reshape(4, 2, d // 8, fq)
            r = send(lax.dynamic_index_in_dim(s, 1 - k, 1, keepdims=False), "dz")
            s = lax.dynamic_index_in_dim(s, k, 1, keepdims=False) + r
            parts = []
            for t in range(4):
                part = lax.dynamic_index_in_dim(s, q ^ t, 0, keepdims=False)
                if t:
                    part = lax.ppermute(part, ("dy", "dx"), [(a, a ^ (0, 2, 1, 3)[t]) for a in range(4)])
                parts.append(part)
            parts = [jnp.where(j == 0, parts[b], parts[b ^ 1]) for b in range(4)]
            return jnp.concatenate([jnp.where(i == 0, parts[b], parts[b ^ 2]) for b in range(4)], axis=1)

        def update(w, m, s, l):
            rws = m.shape[0]
            w_loc = lax.dynamic_slice_in_dim(w, (q * 2 + k) * rws, rws, 0).astype(f32)
            m_new = _row_major(MU * m + s / n)
            w_new = _row_major((w_loc - LR * m_new).astype(bf))
            if l > 2:
                w_new = lax.all_gather(w_new, "dz", axis=0, tiled=True)
                w_new = lax.all_gather(w_new, ("dx", "dy"), axis=0, tiled=True)
            else:
                w_new = lax.all_gather(w_new, DATA, axis=0, tiled=True)
            return _copy(w_new), m_new

        g_x = send(g, "dy")
        g_p = send(g, "dx")
        x_x = send(x, "dy")
        x_p = send(x, "dx")
        z1 = nn(x, w1).astype(bf)
        h1 = act(z1)
        h2 = (nn(h1, w2) + x.astype(f32)).astype(bf)
        h2_x = send(h2, "dy")
        h2_p = send(h2, "dx")
        h1_r = send(cols(h1, qp), "dx")
        g_o = both(g_x)
        h2_o = both(h2_x)
        x_o = both(x_x)
        z3 = nn(h2, w3).astype(bf)
        h3 = act(z3)
        h3_r = send(cols(h3, qp), "dx")
        dz3 = _gelu_grad(z3, nt(g, w4).astype(bf)).astype(bf)
        dz3_r = send(cols(dz3, qp), "dx")
        s4 = tn(cols(h3, q), g) + tn(h3_r, g_p)
        z3_o = nn(h2_o, cols(w3, q)).astype(bf)
        h3_o = act(z3_o)
        s4 = s4 + tn(h3_o, g_o)
        s4 = sum_f(s4)
        dz3_o = _gelu_grad(z3_o, nt(g_o, rows(w4, q)).astype(bf)).astype(bf)
        s3 = tn(h2, cols(dz3, q)) + tn(h2_p, dz3_r)
        s3 = s3 + tn(h2_o, dz3_o)
        s3 = sum_d(s3)
        dh2 = (nt(dz3, w3) + g.astype(f32)).astype(bf)
        dh2_x = send(dh2, "dy")
        dh2_p = send(dh2, "dx")
        dh2_o = both(dh2_x)
        w4n, m4n = update(w4, m4, s4, 4)
        dz1 = _gelu_grad(z1, nt(dh2, w2).astype(bf)).astype(bf)
        dz1_r = send(cols(dz1, qp), "dx")
        w3n, m3n = update(w3, m3, s3, 3)
        z1_o = nn(x_o, cols(w1, q)).astype(bf)
        h1_o = act(z1_o)
        s1 = tn(x, cols(dz1, q)) + tn(x_p, dz1_r)
        dz1_o = _gelu_grad(z1_o, nt(dh2_o, rows(w2, q)).astype(bf)).astype(bf)
        s1 = s1 + tn(x_o, dz1_o)
        s1 = sum_d(s1)
        s2 = tn(cols(h1, q), dh2) + tn(h1_r, dh2_p)
        s2 = s2 + tn(h1_o, dh2_o)
        s2 = sum_f(s2)
        w1n, m1n = update(w1, m1, s1, 1)
        w2n, m2n = update(w2, m2, s2, 2)
        dx = (nt(dz1, w1) + dh2.astype(f32)).astype(bf)
        return (dx, w1n, w2n, w3n, w4n, m1n, m2n, m3n, m4n)

    row, rep = P(DATA, None), P()
    return jax.shard_map(body, mesh=mesh,
                         in_specs=(row, row, rep, rep, rep, rep, row, row, row, row),
                         out_specs=(row, rep, rep, rep, rep, row, row, row, row),
                         check_vma=False)
```

```python
import functools

import jax
import jax.numpy as jnp
from jax import lax
from jax.experimental import pallas as pl
from jax.experimental.pallas import tpu as pltpu
from jax.sharding import PartitionSpec as P


LR = 0.0005
MU = 0.9
DATA = ("dx", "dy", "dz")
f32, bf = jnp.float32, jnp.bfloat16

C0, C1 = 0.7978845608028654, 0.044715


def _gelu(z):
    t = jnp.tanh(C0 * (z + C1 * (z * z * z)))
    return z * (0.5 * t + 0.5)


def _gelu_slope(z):
    z2 = z * z
    t = jnp.tanh(C0 * (z + C1 * (z2 * z)))
    return (0.5 * t + 0.5) + (1.0 - t * t) * (z * (0.5 * C0 + (1.5 * C0 * C1) * z2))


NN = (((1,), (0,)), ((), ()))
NT = (((1,), (1,)), ((), ()))
TN = (((0,), (0,)), ((), ()))


def _dot(a, b, dims):
    return lax.dot_general(a, b, dims, preferred_element_type=f32)


def _params(n):
    return pltpu.CompilerParams(dimension_semantics=("arbitrary",) * n, vmem_limit_bytes=62 * 2**20)


def _cost(m, n, k, size=2):
    return pl.CostEstimate(flops=2 * m * n * k, bytes_accessed=2 * (m * k + k * n) + size * m * n, transcendentals=0)


def _chunks(m, c):
    return [pl.ds(s, c) for s in range(0, m, c)]


def _part(src, dst, at, per):
    @pl.when(jnp.logical_and(at >= 0, at < per))
    def _():
        for r in _chunks(src.shape[0], 256):
            dst[r, :] = src[r, :]


def _zh_body(per, idx, a, w, z, h, *part):
    for r in _chunks(a.shape[0], 512):
        zb = _dot(a[r, :], w[...], NN).astype(bf)
        z[r, :] = zb
        h[r, :] = _gelu(zb.astype(f32)).astype(bf)
    if part:
        _part(h, part[0], pl.program_id(1) - per * idx[1], per)


def _dz_body(per, idx, a, w, z, o, *part):
    for r in _chunks(a.shape[0], 512):
        d = _dot(a[r, :], w[...], NT).astype(bf).astype(f32)
        o[r, :] = (_gelu_slope(z[r, :].astype(f32)) * d).astype(bf)
    if part:
        _part(o, part[0], pl.program_id(1) - per * idx[1], per)


def _expand(kind, idx, a, w, z=None):
    m, d = a.shape
    tm, tn = 2048, 512
    own = m == tm
    f = w.shape[1] if kind == "zh" else w.shape[0]
    per = f // 4 // tn
    width = f if own else f // 4
    col = (lambda i, n, s: n) if own else (lambda i, n, s: s[0] * per + n)
    if kind == "zh":
        w_spec = pl.BlockSpec((d, tn), lambda i, n, s: (0, col(i, n, s)))
    else:
        w_spec = pl.BlockSpec((tn, d), lambda i, n, s: (col(i, n, s), 0))
    tile = pl.BlockSpec((tm, tn), lambda i, n, s: (i, n))
    outs = [tile] * (2 if kind == "zh" else 1)
    shapes = [jax.ShapeDtypeStruct((m, width), bf)] * len(outs)
    if own:
        outs.append(pl.BlockSpec((tm, tn), lambda i, n, s: (0, jnp.clip(n - per * s[1], 0, per - 1))))
        shapes.append(jax.ShapeDtypeStruct((m, f // 4), bf))
    ins = [pl.BlockSpec((tm, d), lambda i, n, s: (i, 0)), w_spec] + ([] if z is None else [tile])
    return pl.pallas_call(
        functools.partial(_zh_body if kind == "zh" else _dz_body, per),
        grid_spec=pltpu.PrefetchScalarGridSpec(num_scalar_prefetch=1, grid=(m // tm, width // tn), in_specs=ins,
                                               out_specs=outs),
        out_shape=shapes, compiler_params=_params(2), cost_estimate=_cost(m, width, d, 4),
    )(idx, a, w, *(() if z is None else (z,)))


def _contract_body(dims, a, w, x, o, acc):
    k = pl.program_id(1)

    @pl.when(k == 0)
    def _():
        for r in _chunks(a.shape[0], 256):
            acc[r, :] = x[r, :].astype(f32)

    for r in _chunks(a.shape[0], 512):
        acc[r, :] += _dot(a[r, :], w[...], dims)

    @pl.when(k == pl.num_programs(1) - 1)
    def _():
        for r in _chunks(a.shape[0], 256):
            o[r, :] = acc[r, :].astype(bf)


def _contract(a, w, x, dims):
    m, f = a.shape
    d = x.shape[1]
    tn, tk = 1024, 2048
    if dims is NN:
        w_spec = pl.BlockSpec((tk, tn), lambda n, k: (k, n))
    else:
        w_spec = pl.BlockSpec((tn, tk), lambda n, k: (n, k))
    tile = pl.BlockSpec((m, tn), lambda n, k: (0, n))
    return pl.pallas_call(
        functools.partial(_contract_body, dims), grid=(d // tn, f // tk),
        in_specs=[pl.BlockSpec((m, tk), lambda n, k: (0, k)), w_spec, tile], out_specs=tile,
        out_shape=jax.ShapeDtypeStruct((m, d), bf), scratch_shapes=[pltpu.VMEM((m, tn), f32)],
        compiler_params=_params(2), cost_estimate=_cost(m, d, f),
    )(a, w, x)


def _grad_body(per, steps, idx, *refs):
    o = refs[-1]
    k = pl.program_id(0)

    @pl.when(k == 0)
    def _():
        for r in _chunks(o.shape[0], 256):
            o[r, :] = jnp.zeros((256, o.shape[1]), f32)

    start = 0
    for s, n in enumerate(steps):
        group = refs[s * (per + 1):(s + 1) * (per + 1)]

        @pl.when(jnp.logical_and(k >= start, k < start + n))
        def _(group=group):
            for t, blk in enumerate(group[:per]):
                wide = blk.shape[1]
                for c in range(0, wide, 512):
                    part = min(wide, 512)
                    o[pl.ds(t * wide + c, part), :] += _dot(blk[:, pl.ds(c, part)], group[per][...], TN)

        start += n


def _grad(idx, sources, a_cols, b_cols, tall):
    tk = 512
    wide = 1024 // tall
    steps = [a.shape[0] // tk for a, _ in sources]
    n_cols = 2048
    specs, args, start = [], [], 0
    for s, (a, b) in enumerate(sources):
        def at(k, start=start, n=steps[s]):
            return jnp.clip(k - start, 0, n - 1)

        for t in range(tall):
            specs.append(pl.BlockSpec((tk, wide), lambda k, i, at=at, s=s, t=t: (at(k), a_cols[s](i, t))))
            args.append(a)
        specs.append(pl.BlockSpec((tk, n_cols), lambda k, i, at=at, s=s: (at(k), b_cols[s](i))))
        args.append(b)
        start += steps[s]
    return pl.pallas_call(
        functools.partial(_grad_body, tall, steps),
        grid_spec=pltpu.PrefetchScalarGridSpec(num_scalar_prefetch=1, grid=(start,), in_specs=specs,
                                               out_specs=pl.BlockSpec((1024, n_cols), lambda k, i: (0, 0))),
        out_shape=jax.ShapeDtypeStruct((1024, n_cols), f32), compiler_params=_params(1),
        cost_estimate=_cost(1024, n_cols, start * tk, 4),
    )(idx, *args)


def _copy_block(src, dst):
    dst[...] = src[...]


def _move(body, grid, idx, ins, in_specs, outs, out_specs):
    size = sum(a.size * a.dtype.itemsize for a in outs)
    return pl.pallas_call(
        body, grid_spec=pltpu.PrefetchScalarGridSpec(num_scalar_prefetch=1, grid=grid, in_specs=in_specs,
                                                     out_specs=out_specs),
        out_shape=outs, compiler_params=_params(len(grid)),
        cost_estimate=pl.CostEstimate(flops=size, bytes_accessed=2 * size, transcendentals=0),
    )(idx, *ins)


def _copy(a):
    r, c = a.shape
    spec = pl.BlockSpec(((1 << 20) // c, c), lambda b: (b, 0))
    return pl.pallas_call(_copy_block, grid=(r * c >> 20,), in_specs=[spec], out_specs=spec,
                          out_shape=jax.ShapeDtypeStruct(a.shape, a.dtype), compiler_params=_params(1),
                          cost_estimate=pl.CostEstimate(flops=r * c, bytes_accessed=4 * r * c, transcendentals=0))(a)


def _deal_body(idx, *refs):
    for t in range(4):
        refs[8 + t][...] = refs[t][...] + refs[4 + t][...]


def _deal(idx, s, r):
    rows, cols = s.shape[0] // 4, s.shape[1]
    tr = 64
    per = rows // tr
    ins = [pl.BlockSpec((tr, cols), lambda b, i, t=t: ((i[0] ^ t) * per + b, 0)) for t in range(4)]
    return _move(_deal_body, (per,), idx, [s] * 4 + [r] * 4, ins * 2,
                 [jax.ShapeDtypeStruct((rows, cols), f32)] * 4, [pl.BlockSpec((tr, cols), lambda b, i: (b, 0))] * 4)


def _step(m, g, w, n, m_new, w_new):
    v = MU * m[...] + g / n
    m_new[...] = v
    w_new[...] = (w[...].astype(f32) - LR * v).astype(bf)


def _update_f_body(n, idx, m, w, s, r, m_new, w_new):
    _step(m, s[...] + r[...], w, n, m_new, w_new)


def _update_d_body(n, idx, m, w, *refs):
    for t in range(4):
        @pl.when(pl.program_id(1) == (idx[0] ^ t))
        def _(t=t):
            _step(m, refs[t][...], w, n, refs[4], refs[5])


def _update(n, idx, m, w, terms):
    rows, cols = m.shape
    outs = [jax.ShapeDtypeStruct(m.shape, f32), jax.ShapeDtypeStruct(m.shape, bf)]
    if len(terms) == 2:
        tr = 128
        per = rows // tr
        tile = pl.BlockSpec((tr, cols), lambda b, i: (b, 0))
        w_tile = pl.BlockSpec((tr, cols), lambda b, i: (i[3] * per + b, 0))
        return _move(functools.partial(_update_f_body, n), (per,), idx, [m, w, *terms],
                     [tile, w_tile, tile, tile], outs, [tile, tile])
    tr, tc = 128, cols // 4
    per = rows // tr
    tile = pl.BlockSpec((tr, tc), lambda b, c, i: (b, c))
    w_tile = pl.BlockSpec((tr, tc), lambda b, c, i: (i[3] * per + b, c))
    term = pl.BlockSpec((tr, tc), lambda b, c, i: (b, 0))
    return _move(functools.partial(_update_d_body, n), (per, 4), idx, [m, w, *terms], [tile, w_tile] + [term] * 4,
                 outs, [tile, tile])


def _join_body(idx, a, b, o):
    mine = pl.program_id(0) == idx[2]

    @pl.when(mine)
    def _():
        o[...] = a[...]

    @pl.when(jnp.logical_not(mine))
    def _():
        o[...] = b[...]


def _join(idx, a, b):
    rows, cols = a.shape
    tr = (1 << 19) // cols
    per = rows // tr
    src = pl.BlockSpec((tr, cols), lambda h, t, i: (t, 0))
    return _move(_join_body, (2, per), idx, [a, b], [src, src], [jax.ShapeDtypeStruct((2 * rows, cols), bf)],
                 [pl.BlockSpec((tr, cols), lambda h, t, i: (h * per + t, 0))])[0]


def solution(mesh):
    ndx, ndy, ndz = mesh.shape["dx"], mesh.shape["dy"], mesh.shape["dz"]
    n = ndx * ndy * ndz
    swap = [(0, 1), (1, 0)]

    def body(x, g, w1, w2, w3, w4, m1, m2, m3, m4):
        i, j, k = lax.axis_index("dx"), lax.axis_index("dy"), lax.axis_index("dz")
        q, qp = 2 * i + j, 2 * (1 - i) + j
        send_idx = jnp.stack([q, qp, 1 - k, 2 * q + k]).astype(jnp.int32)
        keep_idx = jnp.stack([q, qp, k, 2 * q + k]).astype(jnp.int32)

        def send(a, ax):
            return lax.ppermute(a, ax, swap)

        def both(a):
            return lax.all_gather(a, "dx", axis=0, tiled=True)

        def halves(sources, a_cols, b_cols, tall):
            s = _grad(send_idx, sources, a_cols, b_cols, tall)
            r = send(s, "dz")
            s = _grad(keep_idx, sources, a_cols, b_cols, tall)
            return s, r

        def grad_f(h, h_r, h_o, c, c_p, c_o):
            return halves(((h, c), (h_r, c_p), (h_o, c_o)),
                          (lambda v, t: 2 * v[0] + v[2], lambda v, t: v[2], lambda v, t: v[2]), (lambda v: 0,) * 3, 1)

        def grad_d(a, a_p, a_o, z, z_r, z_o):
            s, r = halves(((a, z), (a_p, z_r), (a_o, z_o)), (lambda v, t: 2 * t + v[2],) * 3,
                          (lambda v: v[0], lambda v: 0, lambda v: 0), 4)
            parts = list(_deal(keep_idx, s, r))
            for t in range(1, 4):
                parts[t] = lax.ppermute(parts[t], ("dy", "dx"), [(a, a ^ (0, 2, 1, 3)[t]) for a in range(4)])
            return parts

        def update(w, m, terms, l):
            m_new, w_new = _update(n, keep_idx, m, w, terms)
            if l > 2:
                r = send(w_new, "dz")
                w_new = _join(keep_idx, w_new, r)
                w_new = lax.all_gather(w_new, ("dx", "dy"), axis=0, tiled=True)
            else:
                w_new = lax.all_gather(w_new, DATA, axis=0, tiled=True)
            return _copy(w_new), m_new

        g_x, g_p = send(g, "dy"), send(g, "dx")
        x_x, x_p = send(x, "dy"), send(x, "dx")
        z1, h1, h1_s = _expand("zh", send_idx, x, w1)
        h1_r = send(h1_s, "dx")
        h2 = _contract(h1, w2, x, NN)
        h2_x, h2_p = send(h2, "dy"), send(h2, "dx")
        g_o, h2_o, x_o = both(g_x), both(h2_x), both(x_x)
        z3, h3, h3_s = _expand("zh", send_idx, h2, w3)
        h3_r = send(h3_s, "dx")
        dz3, dz3_s = _expand("dz", send_idx, g, w4, z3)
        dz3_r = send(dz3_s, "dx")
        dh2 = _contract(dz3, w3, g, NT)
        dh2_x, dh2_p = send(dh2, "dy"), send(dh2, "dx")
        dh2_o = both(dh2_x)
        z3_o, h3_o = _expand("zh", send_idx, h2_o, w3)
        s4, r4 = grad_f(h3, h3_r, h3_o, g, g_p, g_o)
        (dz3_o,) = _expand("dz", send_idx, g_o, w4, z3_o)
        s3 = grad_d(h2, h2_p, h2_o, dz3, dz3_r, dz3_o)
        dz1, dz1_s = _expand("dz", send_idx, dh2, w2, z1)
        dz1_r = send(dz1_s, "dx")
        w4n, m4n = update(w4, m4, (s4, r4), 4)
        w3n, m3n = update(w3, m3, s3, 3)
        z1_o, h1_o = _expand("zh", send_idx, x_o, w1)
        (dz1_o,) = _expand("dz", send_idx, dh2_o, w2, z1_o)
        s1 = grad_d(x, x_p, x_o, dz1, dz1_r, dz1_o)
        s2, r2 = grad_f(h1, h1_r, h1_o, dh2, dh2_p, dh2_o)
        w1n, m1n = update(w1, m1, s1, 1)
        w2n, m2n = update(w2, m2, (s2, r2), 2)
        dx = _contract(dz1, w1, dh2, NT)
        return (dx, w1n, w2n, w3n, w4n, m1n, m2n, m3n, m4n)

    row, rep = P(DATA, None), P()
    return jax.shard_map(body, mesh=mesh,
                         in_specs=(row, row, rep, rep, rep, rep, row, row, row, row),
                         out_specs=(row, rep, rep, rep, rep, row, row, row, row),
                         check_vma=False)
```
